32 devices in a mesh: groups: 2 (over y), view: 4 (over z), cuts: 2 (over x), row: 2 (over core).
Axes of the slice: x: 2, y: 2, z: 4, core: 2. Of those that a mesh axis runs over, the one named last changes fastest.
Arguments:
- sinogram: bfloat16 [4, 512, 2048], P('groups', ('view', 'cuts', 'row')), parts along dimension 0, may hold values from -1.5 to 1.5
- leaf_offsets: int32 [512, 512], P('view'), may hold values from 0 to 62
- leaf_frac: float32 [512, 512], P('view'), may hold values from 0 to 1
- merge_offsets: int32 [2, 4096], replicated, may hold values from 0 to 1020, as said below
- merge_weights: float32 [2, 4, 4096], replicated, may hold values from 0.1 to 0.6
Outputs:
- images: float32 [4, 2048, 2048], P(('groups', 'cuts'), ('view', 'row')), parts along dimension 0
The draws below stay inside these ranges and needn't reach their ends.
There are 2 independent parts, one for each index of `groups`. The reference program is written for one: setup_inputs(seed, part) draws one part's arguments, and reference() takes and returns one part's arrays. A program takes and returns all parts, laid end to end along the dimension named above; an argument that names none is the same for every part. Nothing has to cross between parts.
Inputs may be any that keep to these rules, and one draw needn't show every extreme that they name: merge_offsets[l, j] + 4 <= 512 * 2^l.
All inputs are finite; a program needn't handle non-finite values.
Results may differ from the reference program's by a relative error of at most 0.0075.
Values may be sent and summed in bfloat16 or wider, within the bound.
A program may use at most 128 MiB of HBM per device.

```python
import math
import jax
import jax.numpy as jnp
from jax import lax

N = 2048
SHIFT = 32
TAPS = 4
VIEWS = 512
SLICES = 2
LEVELS = 2
C0 = 512
N_VIEW = 4


def draw_merge_offsets(key, part):
    columns = jnp.arange(2 * N, dtype=jnp.int32)[None, :]
    breadths = (C0 * 2 ** jnp.arange(LEVELS, dtype=jnp.int32))[:, None]
    within = columns % (2 * breadths)
    jitter = jax.random.randint(key, (LEVELS, 2 * N), -2, 3, dtype=jnp.int32)
    return jnp.clip(within // 2 - 1 + jitter, 0, breadths - TAPS).astype(jnp.int32)


def set_ends(array, rng, low, top_value):
    place = [jax.random.randint(jax.random.fold_in(rng, axis), (), 0, length) for axis, length in enumerate(array.shape)]
    main_axis = array.shape.index(max(array.shape))
    beside = place[:main_axis] + [(place[main_axis] + 1) % array.shape[main_axis]] + place[main_axis + 1:]
    return array.at[tuple(place)].set(low).at[tuple(beside)].set(top_value)


def steps_of(rng, shape, pieces, low, largest):
    gain = 1.0
    for position, shards_of in pieces:
        draws = jax.random.uniform(jax.random.fold_in(jax.random.fold_in(rng, 6), position), (shards_of,), jnp.float32, low / len(pieces), largest / len(pieces))
        gain = gain * jnp.repeat(jnp.exp(draws), shape[position] // shards_of).reshape((-1,) + (1,) * (len(shape) - 1 - position))
    return gain


def scatter_about(stream_key, shape, deviation, limit, split=(), held_as=jnp.bfloat16):
    array = jax.random.normal(stream_key, shape, jnp.float32) * deviation
    if len(split) > 0:
        array = steps_of(stream_key, shape, split, -0.22, 0.18) * array
    return jnp.clip(array, min=-limit, max=limit).astype(held_as)


def setup_inputs(seed: int = 0, part: int = 0) -> dict:
    arg_keys = jax.random.split(jax.random.key(seed), 6)
    part_keys = jax.random.split(jax.random.fold_in(arg_keys[5], part), 6)
    sinogram = scatter_about(part_keys[0], (SLICES, VIEWS, N), 0.25, 1.5, ((1, 16),))
    leaf_offsets = set_ends(jax.random.randint(arg_keys[1], (VIEWS, C0), 0, 2 * SHIFT - 1), jax.random.fold_in(arg_keys[1], 1), 0, (2 * SHIFT - 1) - 1).astype(jnp.int32)
    leaf_frac = jnp.clip(1.0 * jax.random.uniform(arg_keys[2], (VIEWS, C0), jnp.float32) ** steps_of(arg_keys[2], (VIEWS, C0), ((0, 4),), -0.2, 0.2), 0.0, 1.0)
    merge_offsets = draw_merge_offsets(jax.random.fold_in(arg_keys[5], 71), part)
    merge_weights = jnp.clip(jax.random.uniform(arg_keys[4], (LEVELS, TAPS, 2 * N), jnp.float32, 0.1, 0.6), 0.1, 0.6)
    return dict(sinogram=sinogram, leaf_offsets=leaf_offsets, leaf_frac=leaf_frac, merge_offsets=merge_offsets, merge_weights=merge_weights)


def rounded(values):
    return lax.optimization_barrier(values.astype(jnp.bfloat16)).astype(jnp.float32)


def ramp_matrix(length):
    positions = jnp.arange(length, dtype=jnp.int32)
    distance = positions[:, None] - positions[None, :]
    is_odd = (jnp.abs(distance) % 2) == 1
    spacing = jnp.where(is_odd, distance, 1).astype(jnp.float32)
    entries = jnp.where(distance == 0, 0.25, jnp.where(is_odd, -1.0 / (math.pi * math.pi * spacing * spacing), 0.0))
    return entries.astype(jnp.bfloat16)


def leaf_image(filtered, offsets, fraction):
    padded = jnp.pad(filtered, ((0, 0), (SHIFT, SHIFT)))
    near_weight = rounded(1.0 - fraction)
    far_weight = rounded(fraction)

    def add_tap(tap_number, running):
        shifted = lax.dynamic_slice_in_dim(padded, tap_number, N, 1)
        weights = jnp.where(offsets == tap_number, near_weight, jnp.where(offsets + 1 == tap_number, far_weight, jnp.zeros((), jnp.float32)))
        return running + jnp.dot(shifted.T, weights, precision=lax.Precision.HIGHEST)

    return lax.fori_loop(0, 2 * SHIFT, add_tap, jnp.zeros((N, C0), jnp.float32))


def operators(offsets, weights, groups, breadth):
    offsets = offsets.reshape(groups, 2 * breadth)
    weights = weights.reshape(TAPS, groups, 2 * breadth)
    row_index = jnp.arange(breadth, dtype=jnp.int32)[None, :, None]
    running = jnp.zeros((groups, breadth, 2 * breadth), jnp.float32)
    for tap_number in range(TAPS):
        running = running + jnp.where(row_index == offsets[:, None, :] + tap_number, weights[tap_number][:, None, :], jnp.zeros((), jnp.float32))
    return rounded(running)


def reference(sinogram, leaf_offsets, leaf_frac, merge_offsets, merge_weights):
    ramp = ramp_matrix(N).astype(jnp.float32)
    per_subset = VIEWS // N_VIEW
    subset_offsets = leaf_offsets.reshape(N_VIEW, per_subset, C0)
    subset_fraction = leaf_frac.reshape(N_VIEW, per_subset, C0)

    def one_slice(readings):
        filtered = rounded(jnp.dot(readings.astype(jnp.float32), ramp, precision=lax.Precision.HIGHEST))
        leaves = lax.map(lambda member: leaf_image(member[0], member[1], member[2]), (filtered.reshape(N_VIEW, per_subset, N), subset_offsets, subset_fraction))
        current = rounded(leaves)
        for depth in range(LEVELS):
            breadth = C0 * 2 ** depth
            groups = N_VIEW >> depth
            mapping = operators(merge_offsets[depth], merge_weights[depth], groups, breadth)
            paired = current.reshape(groups // 2, 2, N, breadth)
            paired_maps = mapping.reshape(groups // 2, 2, breadth, 2 * breadth)
            merged = jnp.einsum("gpnw,gpwc->gnc", paired, paired_maps, precision=lax.Precision.HIGHEST)
            current = merged if depth == LEVELS - 1 else rounded(merged)
        return current[0]

    return lax.map(one_slice, sinogram)
```

```python
import functools
import math

import jax
import jax.numpy as jnp
import numpy as np
from jax import lax
from jax.experimental import pallas as pl
from jax.experimental.pallas import tpu as pltpu
from jax.sharding import PartitionSpec as P

SHIFT = 32
TAPS = 4
SPAN = 2 * SHIFT
STEP = 16
MESH = pl.DeviceIdType.MESH


def ramp_band(length, block, window):
    blocks = length // block
    rows = np.arange((2 * blocks - 1) * block)[:, None] - (blocks - 1) * block
    apart = rows + SHIFT - np.arange(window)[None, :]
    odd = np.abs(apart) % 2 == 1
    spacing = np.where(odd, apart, 1).astype(np.float32)
    entries = np.where(
        apart == 0, 0.25, np.where(odd, -1.0 / (math.pi * math.pi * spacing * spacing), 0.0)
    )
    return entries.astype(np.float32).astype(jnp.bfloat16)


def kernel(
    dims,
    sino, offs, frac, moffs, mweights, band_hbm,
    out,
    band, stage, filt, tab, tall, shifted, taps, subs, maps,
    band_sem, send_f, recv_f, send_t, recv_t, send_p, recv_p,
):
    views, cuts, rows, planes, slices, own, length, block, window, per, cols, levels = dims
    group = lax.axis_index("groups")
    view = lax.axis_index("view")
    cut = lax.axis_index("cuts")
    row = lax.axis_index("row")
    members = views * cuts * rows
    sources = cuts * rows
    me = (view * cuts + cut) * rows + row
    part = group * rows + row
    share = per // planes
    bf16 = jnp.bfloat16
    f32 = jnp.float32

    load_band = pltpu.make_async_copy(band_hbm, band, band_sem)
    load_band.start()

    def member_id(d):
        return {"view": d // (cuts * rows), "cuts": (d // rows) % cuts, "row": d % rows}

    def plane_id(p):
        return {"groups": p // rows, "row": p % rows}

    barrier = pltpu.get_barrier_semaphore()

    @pl.loop(1, members)
    def _(k):
        pl.semaphore_signal(
            barrier, inc=1, device_id=member_id((me + k) % members), device_id_type=MESH
        )

    away = planes // rows - 1
    for g in range(1, away + 1):
        for r in range(rows):
            pl.semaphore_signal(
                barrier,
                inc=1,
                device_id={"groups": (group + g) % (away + 1), "row": r},
                device_id_type=MESH,
            )

    for p in range(planes):
        span = pl.ds(p * share, share)
        tab[view, p, 0] = offs[span, :].astype(f32).astype(bf16)
        tab[view, p, 1] = (frac[span, :] - 0.5).astype(bf16)

    pl.semaphore_wait(barrier, members - 1 + away * rows)

    def table_copy(k):
        return pltpu.make_async_remote_copy(
            src_ref=tab.at[view, part],
            dst_ref=tab.at[view, part],
            send_sem=send_t.at[k],
            recv_sem=recv_t.at[view],
            device_id={"view": (view + k) % views},
            device_id_type=MESH,
        )

    @pl.loop(1, views)
    def _(k):
        table_copy(k).start()

    load_band.wait()
    readings = sino[...].astype(f32).reshape(slices * own, length).astype(bf16)
    lane = lax.broadcasted_iota(jnp.int32, (slices * own, window), 1)
    blocks = length // block

    @pl.loop(0, blocks)
    def _(w):
        start = pl.multiple_of((blocks - 1 - w) * block, block)
        value = jnp.dot(readings, band[pl.ds(start, length), :], preferred_element_type=f32)
        place = lane + (w * block - SHIFT)
        value = jnp.where((place >= 0) & (place < length), value, 0.0)
        for s in range(slices):
            stage[((w // rows) * cuts + s) * rows + w % rows] = value[
                s * own : (s + 1) * own
            ].astype(bf16)

    def filtered_copy(k):
        d = (me + k) % members
        return pltpu.make_async_remote_copy(
            src_ref=stage.at[d],
            dst_ref=filt.at[me],
            send_sem=send_f.at[d],
            recv_sem=recv_f.at[me],
            device_id=member_id(d),
            device_id_type=MESH,
        )

    @pl.loop(1, members)
    def _(k):
        filtered_copy(k).start()

    filt[me] = stage[me]

    for level in range(levels):
        width = cols << level
        tile = min(width, 256)
        index = lax.broadcasted_iota(jnp.int32, (tile, tile), 0).astype(f32).astype(bf16)
        count = views >> level
        tiles = 2 * width // tile

        @pl.loop(0, count * tiles)
        def _(i):
            g = i // tiles
            column = pl.multiple_of((i % tiles) * tile, tile)
            at = pl.ds(pl.multiple_of(i * tile, tile), tile)
            offset = moffs[level : level + 1, at].astype(f32)
            weights = [mweights[level, k : k + 1, at].astype(bf16) for k in range(TAPS)]
            for b in range(width // tile):
                near = jnp.clip(offset - float(b * tile), -8.0, float(tile + 8)).astype(bf16)
                apart = index - near
                entry = jnp.zeros((tile, tile), bf16)
                for k in range(TAPS):
                    entry = jnp.where(apart == jnp.asarray(k, bf16), weights[k], entry)
                down = pl.multiple_of((g % 2) * width + b * tile, tile)
                maps[level][g // 2, pl.ds(down, tile), pl.ds(column, tile)] = entry

    def plane_copy(k, m):
        v = (view + k) % views
        return pltpu.make_async_remote_copy(
            src_ref=tab.at[v, part],
            dst_ref=tab.at[v, part],
            send_sem=send_p.at[k, m],
            recv_sem=recv_p.at[v, part],
            device_id=plane_id((part + m) % planes),
            device_id_type=MESH,
        )

    def table_arrival(v, p, sem):
        return pltpu.make_async_remote_copy(
            src_ref=tab.at[v, p],
            dst_ref=tab.at[v, p],
            send_sem=send_t.at[0],
            recv_sem=sem,
            device_id={"view": view},
            device_id_type=MESH,
        )

    @pl.loop(1, views)
    def _(k):
        v = (view + k) % views
        table_arrival(v, part, recv_t.at[v]).wait_recv()
        for m in range(1, planes):
            plane_copy(k, m).start()

    def filtered_arrival(d):
        return pltpu.make_async_remote_copy(
            src_ref=filt.at[d],
            dst_ref=filt.at[d],
            send_sem=send_t.at[0],
            recv_sem=recv_f.at[d],
            device_id={"view": view},
            device_id_type=MESH,
        )

    @pl.loop(0, views)
    def _(k):
        v = (view + k) % views

        @pl.loop(0, sources)
        def _(i):
            d = v * sources + i

            @pl.when(d != me)
            def _():
                filtered_arrival(d).wait_recv()

        @pl.when(k > 0)
        def _():
            for m in range(1, planes):
                p = (part + m) % planes
                table_arrival(v, p, recv_p.at[v, p]).wait_recv()

        rays = filt[pl.ds(v * sources, sources)].astype(f32).reshape(per, window)
        tall[...] = rays.T
        reach = block + SPAN - STEP
        for b in range(STEP):
            shifted[:, b * per : (b + 1) * per] = tall[pl.ds(b, reach), :].astype(bf16)

        tight = min(share, STEP)
        inner = share // tight

        @pl.loop(0, per // tight)
        def _(i):
            span = pl.ds(pl.multiple_of((i % inner) * tight, tight), tight)
            where = tab[v, i // inner, 0, span, :]
            frac_off = tab[v, i // inner, 1, span, :].astype(f32)
            near = (0.5 - frac_off).astype(bf16)
            far = (0.5 + frac_off).astype(bf16)
            zero = jnp.zeros((tight, cols), bf16)
            before = None
            for t in range(SPAN):
                here = where == jnp.asarray(t, bf16)
                entry = zero if before is None else jnp.where(before, far, zero)
                entry = jnp.where(here, near, entry)
                before = here
                down = pl.multiple_of((t % STEP) * per + i * tight, tight)
                taps[t // STEP, pl.ds(down, tight), :] = entry

        total = jnp.zeros((block, cols), f32)
        for a in range(SPAN // STEP):
            total = total + jnp.dot(
                shifted[a * STEP : a * STEP + block, :], taps[a], preferred_element_type=f32
            )
        across = pl.multiple_of((v % 2) * cols, cols)
        subs[0][v // 2, :, pl.ds(across, cols)] = total.astype(bf16)

    for level in range(levels):
        width = cols << level
        tile = min(2 * width, 512)
        tiles = 2 * width // tile
        pairs = views >> (level + 1)
        last = level == levels - 1

        @pl.loop(0, pairs * tiles)
        def _(i):
            g = i // tiles
            column = pl.multiple_of((i % tiles) * tile, tile)
            merged = jnp.dot(
                subs[level][g], maps[level][g, :, pl.ds(column, tile)], preferred_element_type=f32
            )
            if last:
                out[0, :, pl.ds(column, tile)] = merged
            else:
                across = pl.multiple_of((g % 2) * 2 * width + column, tile)
                subs[level + 1][g // 2, :, pl.ds(across, tile)] = merged.astype(bf16)

    @pl.loop(1, members)
    def _(k):
        filtered_copy(k).wait_send()

    @pl.loop(1, views)
    def _(k):
        table_copy(k).wait_send()
        for m in range(1, planes):
            plane_copy(k, m).wait_send()


def body(sinogram, leaf_offsets, leaf_frac, merge_offsets, merge_weights):
    cuts = lax.axis_size("cuts")
    rows = lax.axis_size("row")
    views = lax.axis_size("view")
    planes = lax.axis_size("groups") * rows
    levels = views.bit_length() - 1
    slices, own, length = sinogram.shape
    per, cols = leaf_offsets.shape
    block = length // (rows * views)
    window = -(-(block + SPAN) // 128) * 128
    members = views * cuts * rows
    dims = (views, cuts, rows, planes, slices, own, length, block, window, per, cols, levels)
    band = jnp.asarray(ramp_band(length, block, window))
    vmem = pl.BlockSpec(memory_space=pltpu.VMEM)
    bf16 = jnp.bfloat16
    dma = pltpu.SemaphoreType.DMA
    return pl.pallas_call(
        functools.partial(kernel, dims),
        out_shape=jax.ShapeDtypeStruct((1, block, length), jnp.float32),
        in_specs=[vmem] * 5 + [pl.BlockSpec(memory_space=pl.ANY)],
        out_specs=vmem,
        scratch_shapes=[
            pltpu.VMEM(band.shape, bf16),
            pltpu.VMEM((members, own, window), bf16),
            pltpu.VMEM((members, own, window), bf16),
            pltpu.VMEM((views, planes, 2, per // planes, cols), bf16),
            pltpu.VMEM((window, per), jnp.float32),
            pltpu.VMEM((block + SPAN - STEP, STEP * per), bf16),
            pltpu.VMEM((SPAN // STEP, STEP * per, cols), bf16),
            [pltpu.VMEM((views >> (n + 1), block, cols << (n + 1)), bf16) for n in range(levels)],
            [
                pltpu.VMEM((views >> (n + 1), cols << (n + 1), cols << (n + 1)), bf16)
                for n in range(levels)
            ],
            dma,
            dma((members,)),
            dma((members,)),
            dma((views,)),
            dma((views,)),
            dma((views, planes)),
            dma((views, planes)),
        ],
        compiler_params=pltpu.CompilerParams(
            collective_id=0, has_side_effects=True, vmem_limit_bytes=60 * 1024 * 1024
        ),
    )(sinogram, leaf_offsets, leaf_frac, merge_offsets, merge_weights, band)


def solution(mesh):
    placed = (
        P("groups", ("view", "cuts", "row"), None),
        P("view", None),
        P("view", None),
        P(),
        P(),
    )
    return jax.shard_map(
        body,
        mesh=mesh,
        in_specs=placed,
        out_specs=P(("groups", "cuts"), ("view", "row"), None),
        check_vma=False,
    )
```
